32 devices in a mesh: patch: 8 (over z, y), hidden: 4 (over x, core).
Axes of the slice: x: 2, y: 2, z: 4, core: 2. Of those that a mesh axis runs over, the one named last changes fastest.
Arguments:
- nodes: bfloat16 [16384, 512], P('patch', 'hidden'), may hold values from -6 to 6
- edges: bfloat16 [65536, 512], P(('patch', 'hidden')), may hold values from -6 to 6
- senders: int32 [65536], P(('patch', 'hidden')), may hold values from 0 to 4159
- receivers: int32 [65536], P(('patch', 'hidden')), may hold values from 0 to 2047
- halo_rows: int32 [8, 2, 1024], P('patch'), may hold values from 0 to 2047
- coarse_rows: int32 [8, 8, 8], P('patch'), may hold values from 0 to 63
- edge_count: int32 [32], P(('patch', 'hidden')), may hold values from 1024 to 2048, as said below
- w_edge_in: bfloat16 [1536, 512], replicated, may hold values from -0.15625 to 0.15625
- b_edge_in: float32 [512], replicated, may hold values from -3 to 3
- w_edge_out: bfloat16 [512, 512], replicated, may hold values from -0.25 to 0.25
- b_edge_out: float32 [512], replicated, may hold values from -2 to 2
- edge_gain: float32 [512], replicated, may hold values from 0.5 to 1.5
- edge_shift: float32 [512], replicated, may hold values from -1 to 1
- w_node_in: bfloat16 [1024, 512], replicated, may hold values from -0.1875 to 0.1875
- b_node_in: float32 [512], replicated, may hold values from -3 to 3
- w_node_out: bfloat16 [512, 512], replicated, may hold values from -0.25 to 0.25
- b_node_out: float32 [512], replicated, may hold values from -2 to 2
- node_gain: float32 [512], replicated, may hold values from 0.5 to 1.5
- node_shift: float32 [512], replicated, may hold values from -1 to 1
Outputs:
- nodes_out: bfloat16 [16384, 512], P('patch', 'hidden')
- edges_out: bfloat16 [65536, 512], P(('patch', 'hidden'))
The draws below stay inside these ranges and needn't reach their ends.
Inputs may be any that keep to these rules, and one draw needn't show every extreme that they name: `edge_count`: some block holds 2048 live edges.
All inputs are finite; a program needn't handle non-finite values.
Results may differ from the reference program's by a relative error of at most 0.007.
Values may be sent and summed in bfloat16 or wider, within the bound.
A program may use at most 128 MiB of HBM per device.

```python
import jax
import jax.numpy as jnp
from jax import lax

D = 512
NODE_DEV = 2048
EDGE_DEV = 2048
COARSE_DEV = 64
SLOT = 8
HALO = 1024
PATCHES = 8
SHARDS = 32
NODES = 16384
EDGES = 65536
TABLE = 4160
N_HIDDEN = 4


def draw_edge_count(key, part):
    draw_key, pick_key = jax.random.split(jax.random.fold_in(key, 11))
    counts = jax.random.randint(draw_key, (SHARDS,), EDGE_DEV // 2, EDGE_DEV + 1)
    busiest = jax.random.randint(pick_key, (), 0, SHARDS)
    return jnp.where(jnp.arange(SHARDS) == busiest, EDGE_DEV, counts).astype(jnp.int32)


def with_ends(result, rng, least, high):
    longest = result.shape.index(max(result.shape))
    spots = []
    for shift in (0, 1):
        where = [jax.random.randint(jax.random.fold_in(rng, axis), (), 0, length) for axis, length in enumerate(result.shape)]
        where[longest] = (where[longest] + shift) % result.shape[longest]
        spots.append(tuple(where))
    return result.at[spots[0]].set(least).at[spots[1]].set(high)


def shard_levels(own_key, dims, shards, least, high):
    def one(dim, parts):
        steps = jax.random.uniform(jax.random.fold_in(jax.random.fold_in(own_key, 6), dim), (parts,), jnp.float32, least / len(shards), high / len(shards))
        return jnp.repeat(jnp.exp(steps), dims[dim] // parts).reshape((-1,) + (1,) * (len(dims) - dim - 1))

    loudness = one(*shards[0])
    for cut in shards[1:]:
        loudness = loudness * one(*cut)
    return loudness


def gaussian(own_key, shape, deviation, most, pieces=(), kind=jnp.bfloat16):
    result = deviation * jax.random.normal(own_key, shape, jnp.float32)
    if pieces:
        result = result * shard_levels(own_key, shape, pieces, -0.22, 0.18)
    return jnp.clip(result, -most, most).astype(kind)


def setup_inputs(seed: int = 0) -> dict:
    seeds = jax.random.split(jax.random.key(seed), 20)
    nodes = gaussian(seeds[0], (NODES, D), 1.0, 6.0, ((0, 8), (1, 4)))
    edges = gaussian(seeds[1], (EDGES, D), 1.0, 6.0, ((0, 32),))
    senders = with_ends(jax.random.randint(seeds[2], (EDGES,), 0, TABLE), jax.random.fold_in(seeds[2], 1), 0, TABLE - 1).astype(jnp.int32)
    receivers = with_ends(jax.random.randint(seeds[3], (EDGES,), 0, NODE_DEV), jax.random.fold_in(seeds[3], 1), 0, NODE_DEV - 1).astype(jnp.int32)
    halo_rows = with_ends(jax.random.randint(seeds[4], (PATCHES, 2, HALO), 0, NODE_DEV), jax.random.fold_in(seeds[4], 1), 0, NODE_DEV - 1).astype(jnp.int32)
    coarse_rows = with_ends(jax.random.randint(seeds[5], (PATCHES, PATCHES, SLOT), 0, COARSE_DEV), jax.random.fold_in(seeds[5], 1), 0, COARSE_DEV - 1).astype(jnp.int32)
    edge_count = draw_edge_count(jax.random.fold_in(seeds[19], 71), 0)
    w_edge_in = gaussian(seeds[7], (3 * D, D), (3 * D) ** -0.5, 0.15625)
    b_edge_in = gaussian(seeds[8], (D,), 0.5, 3.0, (), jnp.float32)
    w_edge_out = gaussian(seeds[9], (D, D), D ** -0.5, 0.25)
    b_edge_out = gaussian(seeds[10], (D,), 0.3, 2.0, (), jnp.float32)
    edge_gain = jnp.clip(1.0 + 0.1 * jax.random.normal(seeds[11], (D,), jnp.float32), 0.5, 1.5)
    edge_shift = gaussian(seeds[12], (D,), 0.2, 1.0, (), jnp.float32)
    w_node_in = gaussian(seeds[13], (2 * D, D), (2 * D) ** -0.5, 0.1875)
    b_node_in = gaussian(seeds[14], (D,), 0.5, 3.0, (), jnp.float32)
    w_node_out = gaussian(seeds[15], (D, D), D ** -0.5, 0.25)
    b_node_out = gaussian(seeds[16], (D,), 0.3, 2.0, (), jnp.float32)
    node_gain = jnp.clip(1.0 + 0.1 * jax.random.normal(seeds[17], (D,), jnp.float32), 0.5, 1.5)
    node_shift = gaussian(seeds[18], (D,), 0.2, 1.0, (), jnp.float32)
    return {"nodes": nodes, "edges": edges, "senders": senders, "receivers": receivers, "halo_rows": halo_rows, "coarse_rows": coarse_rows, "edge_count": edge_count, "w_edge_in": w_edge_in, "b_edge_in": b_edge_in, "w_edge_out": w_edge_out, "b_edge_out": b_edge_out, "edge_gain": edge_gain, "edge_shift": edge_shift, "w_node_in": w_node_in, "b_node_in": b_node_in, "w_node_out": w_node_out, "b_node_out": b_node_out, "node_gain": node_gain, "node_shift": node_shift}


layer_epsilon = 1e-05

def perceptron(inputs, weight_in, bias_in, weight_out, bias_out, norm_gain, norm_shift):
    joined = jnp.concatenate(inputs, axis=1)
    hidden = jnp.dot(joined, weight_in, preferred_element_type=jnp.float32) + bias_in
    active = jax.nn.silu(hidden).astype(jnp.bfloat16)
    output = jnp.dot(active, weight_out, preferred_element_type=jnp.float32) + bias_out
    row_mean = lax.optimization_barrier(jnp.mean(output, axis=1, keepdims=True))
    row_var = lax.optimization_barrier(jnp.mean(jnp.square(output - row_mean), axis=1, keepdims=True))
    return (output - row_mean) * lax.rsqrt(row_var + layer_epsilon) * norm_gain + norm_shift

def block_segments(values, targets):
    return jax.ops.segment_sum(values, targets, num_segments=NODE_DEV)

def reference(nodes, edges, senders, receivers, halo_rows, coarse_rows, edge_count, w_edge_in, b_edge_in, w_edge_out, b_edge_out, edge_gain, edge_shift, w_node_in, b_node_in, w_node_out, b_node_out, node_gain, node_shift):
    patch_edges = N_HIDDEN * EDGE_DEV

    def patch_work(patch_id):
        first_edge = patch_id * patch_edges
        latent = lax.dynamic_slice_in_dim(edges, first_edge, patch_edges, 0)
        sender_code = lax.dynamic_slice_in_dim(senders, first_edge, patch_edges, 0)
        target = lax.dynamic_slice_in_dim(receivers, first_edge, patch_edges, 0)
        counts = lax.dynamic_slice_in_dim(edge_count, patch_id * N_HIDDEN, N_HIDDEN, 0)
        previous = jnp.mod(patch_id - 1, PATCHES).astype(jnp.int32)
        following = jnp.mod(patch_id + 1, PATCHES).astype(jnp.int32)
        from_previous = halo_rows[previous, 1][jnp.clip(sender_code - NODE_DEV, 0, HALO - 1)]
        from_following = halo_rows[following, 0][jnp.clip(sender_code - NODE_DEV - HALO, 0, HALO - 1)]
        far_slot = jnp.clip(sender_code - NODE_DEV - 2 * HALO, 0, PATCHES * SLOT - 1)
        far_owner = far_slot // SLOT
        far_row = coarse_rows[patch_id][far_owner, far_slot % SLOT]
        source = jnp.where(sender_code < NODE_DEV, patch_id * NODE_DEV + sender_code, jnp.where(sender_code < NODE_DEV + HALO, previous * NODE_DEV + from_previous, jnp.where(sender_code < NODE_DEV + 2 * HALO, following * NODE_DEV + from_following, far_owner * NODE_DEV + far_row))).astype(jnp.int32)
        sender_rows = nodes[source]
        patch_nodes = lax.dynamic_slice_in_dim(nodes, patch_id * NODE_DEV, NODE_DEV, 0)
        receiver_rows = patch_nodes[target]
        update = perceptron((latent, sender_rows, receiver_rows), w_edge_in, b_edge_in, w_edge_out, b_edge_out, edge_gain, edge_shift)
        position = jnp.arange(patch_edges, dtype=jnp.int32)
        live_mask = position % EDGE_DEV < counts[position // EDGE_DEV]
        message = jnp.where(live_mask[:, None], update, jnp.zeros_like(update))
        new_latent = (latent.astype(jnp.float32) + message).astype(jnp.bfloat16)
        sent = lax.optimization_barrier(message.astype(jnp.bfloat16)).astype(jnp.float32)
        partial_sums = jax.vmap(block_segments)(sent.reshape(N_HIDDEN, EDGE_DEV, D), target.reshape(N_HIDDEN, EDGE_DEV))
        rounded = lax.optimization_barrier(partial_sums.astype(jnp.bfloat16)).astype(jnp.float32)
        node_sums = lax.optimization_barrier(jnp.sum(rounded, axis=0))
        return (new_latent, node_sums)
    new_edges, node_sums = lax.map(patch_work, jnp.arange(PATCHES, dtype=jnp.int32))
    edges_out = new_edges.reshape(EDGES, D)
    gathered = node_sums.reshape(NODES, D).astype(jnp.bfloat16)
    update = perceptron((nodes, gathered), w_node_in, b_node_in, w_node_out, b_node_out, node_gain, node_shift)
    nodes_out = (nodes.astype(jnp.float32) + update).astype(jnp.bfloat16)
    return (nodes_out, edges_out)
```

```python
import functools

import jax
import jax.numpy as jnp
from jax import lax
from jax.experimental import pallas as pl
from jax.experimental.pallas import tpu as pltpu
from jax.sharding import PartitionSpec as P

layer_epsilon = 1e-05
MESH = pl.DeviceIdType.MESH
f32 = jnp.float32
bf16 = jnp.bfloat16


def normalize(output, norm_gain, norm_shift):
    row_mean = jnp.mean(output, axis=1, keepdims=True)
    centered = output - row_mean
    row_var = jnp.mean(jnp.square(centered), axis=1, keepdims=True)
    return centered * lax.rsqrt(row_var + layer_epsilon) * norm_gain + norm_shift


def silu(value):
    half = 0.5 * value
    return half + half * jnp.tanh(half)


def dot(a, b):
    return jnp.dot(a, b, preferred_element_type=f32)


def onehot_of(column, start, count):
    ids = lax.broadcasted_iota(jnp.int32, (column.shape[0], count), 1) + start
    return jnp.where(column == ids, 1.0, 0.0).astype(bf16)


def kernel(
    patches, slot, border, block,
    nodes, halo_col, coarse, live, recv_row, vecs,
    send_hbm, recv_hbm, edges_hbm, w_ei_hbm, w_eo_hbm, w_ni_hbm, w_no_hbm,
    nodes_out, edges_out,
    table, stage, req, rep, far_in, far_out, send_col, recv_col, edges,
    w_ei, w_eo, w_ni, w_no, pre, own_send, msg,
    give_far, got_far, give_cross, got_cross, give_near, got_near, fresh,
    load_sem, own_sem, store_sem, ag_send, ag_recv, halo_send, halo_recv,
    req_send, req_recv, rep_send, rep_recv, rs_send, rs_recv, out_send, out_recv,
):
    p = lax.axis_index("patch")
    h = lax.axis_index("hidden")
    near = h + 1 - 2 * lax.rem(h, 2)
    cross = lax.rem(h + 2, 4)
    diag = lax.rem(near + 2, 4)
    rows, cols = nodes.shape
    width = edges.shape[1]
    count = edges.shape[0]
    far = patches * slot
    after = lax.rem(p + 1, patches)
    before = lax.rem(p + patches - 1, patches)

    loads = [
        pltpu.make_async_copy(source, target, load_sem.at[i])
        for i, (source, target) in enumerate((
            (edges_hbm, edges), (recv_hbm, recv_col), (send_hbm, send_col),
            (w_ei_hbm, w_ei), (w_eo_hbm, w_eo), (w_ni_hbm, w_ni), (w_no_hbm, w_no),
        ))
    ]
    for load in loads:
        load.start()

    def mine(index):
        return pl.ds(pl.multiple_of(index * cols, cols), cols)

    barrier = pltpu.get_barrier_semaphore()
    for step in range(1, patches):
        pl.semaphore_signal(
            barrier, inc=1, device_id={"patch": lax.rem(p + step, patches)}, device_id_type=MESH
        )
    for peer in (near, cross, diag):
        pl.semaphore_signal(barrier, inc=1, device_id={"hidden": peer}, device_id_type=MESH)
    pl.semaphore_wait(barrier, patches - 1 + 3)

    def remote(source, target, s_sem, r_sem, device):
        return pltpu.make_async_remote_copy(
            src_ref=source, dst_ref=target, send_sem=s_sem, recv_sem=r_sem,
            device_id=device, device_id_type=MESH,
        )

    def slots(index):
        return pl.ds(pl.multiple_of(index * slot, slot), slot)

    asks = []
    for step in range(1, patches):
        owner = lax.rem(p + step, patches)
        ask = remote(
            coarse.at[slots(owner)], req.at[slots(p)],
            req_send.at[step - 1], req_recv.at[step - 1], {"patch": owner},
        )
        ask.start()
        asks.append(ask)

    half = rows // 2
    spans = [(0, half), (half, half), (rows, border), (rows + border, border), (rows + 2 * border, far)]

    def exchange(k, source):
        start, size = spans[k]
        span = pl.ds(start, size)
        pair = []
        for j, peer in ((1, cross), (0, near)):
            copy = remote(
                source, table.at[span, mine(h)], ag_send.at[k, j], ag_recv.at[k, j], {"hidden": peer}
            )
            copy.start()
            pair.append(copy)
        return pair

    def forward(k):
        start, size = spans[k]
        piece = table.at[pl.ds(start, size), mine(cross)]
        copy = remote(piece, piece, ag_send.at[k, 2], ag_recv.at[k, 2], {"hidden": near})
        copy.start()
        return copy

    pairs = [exchange(0, nodes.at[pl.ds(0, half)]), exchange(1, nodes.at[pl.ds(half, half)])]
    keep = pltpu.make_async_copy(nodes, table.at[pl.ds(0, rows), mine(h)], own_sem.at[0])
    keep.start()
    req[slots(p), :] = coarse[slots(p), :]
    pad = table.shape[0] - rows - 2 * border - far
    if pad:
        table[pl.ds(rows + 2 * border + far, pad), :] = jnp.zeros((pad, width), bf16)

    halos = []
    for side, target, start in ((1, after, rows), (0, before, rows + border)):
        part = pl.ds(side * border, border)
        picked = onehot_of(halo_col[part, :], 0, rows)
        stage[part, :] = dot(picked, nodes[...]).astype(bf16)
        copy = remote(
            stage.at[part], table.at[pl.ds(start, border), mine(h)],
            halo_send.at[side], halo_recv.at[side], {"patch": target},
        )
        copy.start()
        halos.append(copy)

    for ask in asks:
        ask.wait()
    rep[...] = dot(onehot_of(req[...][:, :1], 0, rows), nodes[...])
    answers = []
    for step in range(1, patches):
        reader = lax.rem(p + step, patches)
        answer = remote(
            rep.at[slots(reader)], far_in.at[slots(p)],
            rep_send.at[step - 1], rep_recv.at[step - 1], {"patch": reader},
        )
        answer.start()
        answers.append(answer)
    far_in[slots(p), :] = rep[slots(p), :]

    keep.wait()
    forwards = []
    for pair in pairs:
        pair[0].wait()
        forwards.append(forward(len(forwards)))
    for answer in answers:
        answer.wait()
    far_out[...] = far_in[...].astype(bf16)
    for i, copy in enumerate(halos):
        copy.wait()
        start, size = spans[2 + i]
        pairs.append(exchange(2 + i, table.at[pl.ds(start, size), mine(h)]))
    pairs.append(exchange(4, far_out))
    keep = pltpu.make_async_copy(
        far_out, table.at[pl.ds(rows + 2 * border, far), mine(h)], own_sem.at[1]
    )
    keep.start()
    for i in range(2):
        pairs[i][1].wait()
        forwards[i].wait()
    for load in loads[:4]:
        load.wait()

    def first(step, carry):
        part = pl.ds(pl.multiple_of(step * block, block), block)
        receiver_rows = dot(onehot_of(recv_col[part, :], 0, rows), table[pl.ds(0, rows), :]).astype(bf16)
        own_send[part, :] = dot(
            onehot_of(send_col[part, :], 0, rows), table[pl.ds(0, rows), :]
        ).astype(bf16)
        pre[part, :] = (
            dot(edges[part, :], w_ei[pl.ds(0, width), :])
            + dot(receiver_rows, w_ei[pl.ds(2 * width, width), :])
            + vecs[0:1, :]
        )
        return carry

    lax.fori_loop(0, count // block, first, 0)

    keep.wait()
    for k in (2, 3, 4):
        pairs[k][0].wait()
        forwards.append(forward(k))
    for k in (2, 3, 4):
        pairs[k][1].wait()
        forwards[k].wait()
    for load in loads[4:]:
        load.wait()
    rest = table.shape[0] - rows

    def second(step, carry):
        part = pl.ds(pl.multiple_of(step * block, block), block)
        other = dot(onehot_of(send_col[part, :], rows, rest), table[pl.ds(rows, rest), :])
        sender_rows = (other + own_send[part, :].astype(f32)).astype(bf16)
        active = silu(pre[part, :] + dot(sender_rows, w_ei[pl.ds(width, width), :])).astype(bf16)
        output = dot(active, w_eo[...]) + vecs[1:2, :]
        update = normalize(output, vecs[2:3, :], vecs[3:4, :])
        position = lax.broadcasted_iota(jnp.int32, (block, 1), 0) + step * block
        message = jnp.where(position < live[...], update, 0.0)
        msg[part, :] = message.astype(bf16)
        edges[part, :] = (edges[part, :].astype(f32) + message).astype(bf16)
        return carry

    lax.fori_loop(0, count // block, second, 0)
    save = pltpu.make_async_copy(edges, edges_out, store_sem.at[0])
    save.start()

    share = rows // 4

    def sums(owner):
        ids = lax.broadcasted_iota(jnp.int32, (share, count), 0) + owner * share
        return dot(jnp.where(recv_row[...] == ids, 1.0, 0.0).astype(bf16), msg[...])

    give_far[...] = sums(diag).astype(bf16)
    to_far = remote(give_far, got_far, rs_send.at[0], rs_recv.at[0], {"hidden": near})
    to_far.start()
    pre[pl.ds(0, share), :] = sums(cross)
    to_far.wait()
    cut = share // 2
    to_cross = []
    for i in range(2):
        part = pl.ds(i * cut, cut)
        give_cross[part, :] = (pre[part, :] + got_far[part, :].astype(f32)).astype(bf16)
        copy = remote(
            give_cross.at[part], got_cross.at[part], rs_send.at[1 + i], rs_recv.at[1 + i], {"hidden": cross}
        )
        copy.start()
        to_cross.append(copy)
    give_near[...] = sums(near).astype(bf16)
    to_near = remote(give_near, got_near, rs_send.at[3], rs_recv.at[3], {"hidden": near})
    to_near.start()
    pre[pl.ds(0, share), :] = sums(h)
    own_rows = pl.ds(pl.multiple_of(h * share, share), share)
    pre[pl.ds(share, share), :] = (
        dot(table[own_rows, :], w_ni[pl.ds(0, width), :]) + vecs[4:5, :]
    )
    to_near.wait()
    outs = []
    for i in range(2):
        part = pl.ds(i * cut, cut)
        to_cross[i].wait()
        total = pre[part, :] + got_near[part, :].astype(f32) + got_cross[part, :].astype(f32)
        node_pre = pre[pl.ds(share + i * cut, cut), :] + dot(
            total.astype(bf16), w_ni[pl.ds(width, width), :]
        )
        output = dot(silu(node_pre).astype(bf16), w_no[...]) + vecs[5:6, :]
        update = normalize(output, vecs[6:7, :], vecs[7:8, :])
        place = pl.ds(pl.multiple_of(h * share + i * cut, cut), cut)
        fresh[part, :] = (table[place, :].astype(f32) + update).astype(bf16)
        for j, peer in enumerate((cross, diag, near)):
            copy = remote(
                fresh.at[part, mine(peer)], nodes_out.at[place, :],
                out_send.at[i, j], out_recv.at[i, j], {"hidden": peer},
            )
            copy.start()
            outs.append(copy)
        nodes_out[place, :] = fresh[part, mine(h)]
    for copy in outs:
        copy.wait()
    save.wait()


def local(
    nodes, edges, senders, receivers, halo_rows, coarse_rows, edge_count,
    w_edge_in, b_edge_in, w_edge_out, b_edge_out, edge_gain, edge_shift,
    w_node_in, b_node_in, w_node_out, b_node_out, node_gain, node_shift,
    *, patches,
):
    rows, cols = nodes.shape
    count, width = edges.shape
    border = halo_rows.shape[2]
    slot = coarse_rows.shape[2]
    far = patches * slot
    table_rows = -(-(rows + 2 * border + far) // 256) * 256
    share = rows // 4
    block = min(512, count)
    vecs = jnp.stack([
        b_edge_in, b_edge_out, edge_gain, edge_shift, b_node_in, b_node_out, node_gain, node_shift
    ])
    coarse = jnp.broadcast_to(coarse_rows.reshape(far, 1), (far, 128))
    vmem = pl.BlockSpec(memory_space=pltpu.VMEM)
    hbm = pl.BlockSpec(memory_space=pl.ANY)
    dma = pltpu.SemaphoreType.DMA
    return pl.pallas_call(
        functools.partial(kernel, patches, slot, border, block),
        out_shape=(
            jax.ShapeDtypeStruct((rows, cols), bf16),
            jax.ShapeDtypeStruct((count, width), bf16),
        ),
        in_specs=[vmem] * 6 + [hbm] * 7,
        out_specs=(vmem, hbm),
        scratch_shapes=[
            pltpu.VMEM((table_rows, width), bf16),
            pltpu.VMEM((2 * border, cols), bf16),
            pltpu.VMEM((far, 128), jnp.int32),
            pltpu.VMEM((far, cols), f32),
            pltpu.VMEM((far, cols), f32),
            pltpu.VMEM((far, cols), bf16),
            pltpu.VMEM((count, 1), jnp.int32),
            pltpu.VMEM((count, 1), jnp.int32),
            pltpu.VMEM((count, width), bf16),
            pltpu.VMEM(w_edge_in.shape, bf16),
            pltpu.VMEM(w_edge_out.shape, bf16),
            pltpu.VMEM(w_node_in.shape, bf16),
            pltpu.VMEM(w_node_out.shape, bf16),
            pltpu.VMEM((count, width), f32),
            pltpu.VMEM((count, width), bf16),
            pltpu.VMEM((count, width), bf16),
        ] + [pltpu.VMEM((share, width), bf16)] * 7 + [
            dma((7,)), dma((2,)), dma((1,)), dma((5, 3)), dma((5, 3)), dma((2,)), dma((2,)),
            dma((patches - 1,)), dma((patches - 1,)), dma((patches - 1,)), dma((patches - 1,)),
            dma((4,)), dma((4,)), dma((2, 3)), dma((2, 3)),
        ],
        compiler_params=pltpu.CompilerParams(
            collective_id=0, has_side_effects=True, vmem_limit_bytes=60 * 1024 * 1024
        ),
    )(
        nodes, halo_rows.reshape(-1, 1), coarse, edge_count.reshape(1, 1),
        receivers.reshape(1, -1), vecs,
        senders.reshape(-1, 1), receivers.reshape(-1, 1), edges,
        w_edge_in, w_edge_out, w_node_in, w_node_out,
    )


def solution(mesh):
    spread = P(("patch", "hidden"))
    return jax.shard_map(
        functools.partial(local, patches=mesh.shape["patch"]),
        mesh=mesh,
        in_specs=(
            P("patch", "hidden"), P(("patch", "hidden"), None), spread, spread,
            P("patch", None, None), P("patch", None, None), spread,
        ) + (P(),) * 12,
        out_specs=(P("patch", "hidden"), P(("patch", "hidden"), None)),
        check_vma=False,
    )
```

```python
import functools

import jax
import jax.numpy as jnp
from jax import lax
from jax.experimental import pallas as pl
from jax.experimental.pallas import tpu as pltpu
from jax.sharding import PartitionSpec as P

layer_epsilon = 1e-05
MESH = pl.DeviceIdType.MESH
f32 = jnp.float32
bf16 = jnp.bfloat16


def normalize(output, norm_gain, norm_shift):
    row_mean = jnp.mean(output, axis=1, keepdims=True)
    centered = output - row_mean
    row_var = jnp.mean(jnp.square(centered), axis=1, keepdims=True)
    return centered * lax.rsqrt(row_var + layer_epsilon) * norm_gain + norm_shift


def silu(value):
    half = 0.5 * value
    return half + half * jnp.tanh(half)


def dot(a, b):
    return jnp.dot(a, b, preferred_element_type=f32)


def column_of(row):
    return jnp.transpose(jnp.broadcast_to(row, (128, row.shape[1])))[:, :1]


def onehot_of(column, start, count):
    ids = lax.broadcasted_iota(jnp.int32, (column.shape[0], count), 1) + start
    return jnp.where(column == ids, 1.0, 0.0).astype(bf16)


def kernel(
    patches, slot, border, block,
    nodes, halo, coarse, live, send_row, recv_row,
    b_ei, b_eo, e_gain, e_shift, b_ni, b_no, n_gain, n_shift,
    edges_hbm, w_ei_hbm, w_eo_hbm, w_ni_hbm, w_no_hbm,
    nodes_out, edges_out,
    table, stage, req, rep, far_in, far_out, send_col, recv_col, edges,
    w_ei, w_eo, w_ni, w_no, pre, own_send, msg,
    give_far, got_far, give_cross, got_cross, give_near, got_near, fresh,
    load_sem, own_sem, store_sem, ag_send, ag_recv, halo_send, halo_recv,
    req_send, req_recv, rep_send, rep_recv, rs_send, rs_recv, out_send, out_recv,
):
    p = lax.axis_index("patch")
    h = lax.axis_index("hidden")
    near = h + 1 - 2 * lax.rem(h, 2)
    cross = lax.rem(h + 2, 4)
    diag = lax.rem(near + 2, 4)
    rows, cols = nodes.shape
    width = edges.shape[1]
    count = edges.shape[0]
    far = patches * slot
    after = lax.rem(p + 1, patches)
    before = lax.rem(p + patches - 1, patches)

    loads = [
        pltpu.make_async_copy(source, target, load_sem.at[i])
        for i, (source, target) in enumerate((
            (edges_hbm, edges), (w_ei_hbm, w_ei), (w_eo_hbm, w_eo), (w_ni_hbm, w_ni),
            (w_no_hbm, w_no),
        ))
    ]
    for load in loads:
        load.start()

    def mine(index):
        return pl.ds(pl.multiple_of(index * cols, cols), cols)

    barrier = pltpu.get_barrier_semaphore()
    for step in range(1, patches):
        pl.semaphore_signal(
            barrier, inc=1, device_id={"patch": lax.rem(p + step, patches)}, device_id_type=MESH
        )
    for peer in (near, cross, diag):
        pl.semaphore_signal(barrier, inc=1, device_id={"hidden": peer}, device_id_type=MESH)
    pl.semaphore_wait(barrier, patches - 1 + 3)

    def remote(source, target, s_sem, r_sem, device):
        return pltpu.make_async_remote_copy(
            src_ref=source, dst_ref=target, send_sem=s_sem, recv_sem=r_sem,
            device_id=device, device_id_type=MESH,
        )

    def slots(index):
        return pl.ds(pl.multiple_of(index * slot, slot), slot)

    asks = []
    for step in range(1, patches):
        owner = lax.rem(p + step, patches)
        ask = remote(
            coarse.at[slots(owner)], req.at[slots(p)],
            req_send.at[step - 1], req_recv.at[step - 1], {"patch": owner},
        )
        ask.start()
        asks.append(ask)

    half = rows // 2
    piece_rows = border // 2
    spans = [(0, half), (half, half)]
    for i in range(2):
        spans.append((rows + i * piece_rows, piece_rows))
        spans.append((rows + border + i * piece_rows, piece_rows))
    spans.append((rows + 2 * border, far))

    def exchange(k, source):
        start, size = spans[k]
        span = pl.ds(start, size)
        pair = []
        for j, peer in ((1, cross), (0, near)):
            copy = remote(
                source, table.at[span, mine(h)], ag_send.at[k, j], ag_recv.at[k, j], {"hidden": peer}
            )
            copy.start()
            pair.append(copy)
        return pair

    def forward(k):
        start, size = spans[k]
        piece = table.at[pl.ds(start, size), mine(cross)]
        copy = remote(piece, piece, ag_send.at[k, 2], ag_recv.at[k, 2], {"hidden": near})
        copy.start()
        return copy

    pairs = [exchange(0, nodes.at[pl.ds(0, half)]), exchange(1, nodes.at[pl.ds(half, half)])]
    keep = pltpu.make_async_copy(nodes, table.at[pl.ds(0, rows), mine(h)], own_sem.at[0])
    keep.start()
    req[slots(p), :] = coarse[slots(p), :]
    pad = table.shape[0] - rows - 2 * border - far
    if pad:
        table[pl.ds(rows + 2 * border + far, pad), :] = jnp.zeros((pad, width), bf16)

    halos = []
    for i in range(2):
        for side, target in ((1, after), (0, before)):
            k = len(halos)
            start, size = spans[2 + k]
            held = pl.ds(k * piece_rows, piece_rows)
            ids = column_of(halo[side : side + 1, i * piece_rows : (i + 1) * piece_rows])
            stage[held, :] = dot(onehot_of(ids, 0, rows), nodes[...]).astype(bf16)
            copy = remote(
                stage.at[held], table.at[pl.ds(start, size), mine(h)],
                halo_send.at[k], halo_recv.at[k], {"patch": target},
            )
            copy.start()
            halos.append(copy)

    for ask in asks:
        ask.wait()
    rep[...] = dot(onehot_of(req[...][:, :1], 0, rows), nodes[...])
    answers = []
    for step in range(1, patches):
        reader = lax.rem(p + step, patches)
        answer = remote(
            rep.at[slots(reader)], far_in.at[slots(p)],
            rep_send.at[step - 1], rep_recv.at[step - 1], {"patch": reader},
        )
        answer.start()
        answers.append(answer)
    far_in[slots(p), :] = rep[slots(p), :]

    keep.wait()
    recv_col[...] = column_of(recv_row[...])
    send_col[...] = column_of(send_row[...])
    for load in loads[:2]:
        load.wait()

    def begin(step, carry):
        part = pl.ds(pl.multiple_of(step * block, block), block)
        pre[part, :] = dot(edges[part, :], w_ei[pl.ds(0, width), :]) + b_ei[...]
        return carry

    lax.fori_loop(0, count // block, begin, 0)

    def relay(k):
        halos[k].wait()
        start, size = spans[2 + k]
        pairs.append(exchange(2 + k, table.at[pl.ds(start, size), mine(h)]))

    relay(0)
    relay(1)
    pairs[0][0].wait()
    forwards = [forward(0)]
    relay(2)
    pairs[1][0].wait()
    forwards.append(forward(1))
    for answer in answers:
        answer.wait()
    far_out[...] = far_in[...].astype(bf16)
    far_pair = exchange(6, far_out)
    keep = pltpu.make_async_copy(
        far_out, table.at[pl.ds(rows + 2 * border, far), mine(h)], own_sem.at[1]
    )
    keep.start()
    for i in range(2):
        pairs[i][1].wait()
        forwards[i].wait()

    def first(step, carry):
        part = pl.ds(pl.multiple_of(step * block, block), block)
        receiver_rows = dot(onehot_of(recv_col[part, :], 0, rows), table[pl.ds(0, rows), :]).astype(bf16)
        own_send[part, :] = dot(
            onehot_of(send_col[part, :], 0, rows), table[pl.ds(0, rows), :]
        ).astype(bf16)
        pre[part, :] = pre[part, :] + dot(receiver_rows, w_ei[pl.ds(2 * width, width), :])
        return carry

    steps = count // block
    lax.fori_loop(0, 1, first, 0)
    relay(3)
    pairs.append(far_pair)
    lax.fori_loop(1, steps - 1, first, 0)
    for k in (2, 3, 4):
        pairs[k][0].wait()
        forwards.append(forward(k))
    lax.fori_loop(steps - 1, steps, first, 0)

    keep.wait()
    for k in (6, 5):
        pairs[k][0].wait()
        forwards.append(forward(k))
    for k in range(2, 7):
        pairs[k][1].wait()
    for copy in forwards[2:]:
        copy.wait()
    for load in loads[2:]:
        load.wait()
    rest = table.shape[0] - rows

    def second(step, carry):
        part = pl.ds(pl.multiple_of(step * block, block), block)
        other = dot(onehot_of(send_col[part, :], rows, rest), table[pl.ds(rows, rest), :])
        sender_rows = (other + own_send[part, :].astype(f32)).astype(bf16)
        active = silu(pre[part, :] + dot(sender_rows, w_ei[pl.ds(width, width), :])).astype(bf16)
        output = dot(active, w_eo[...]) + b_eo[...]
        update = normalize(output, e_gain[...], e_shift[...])
        position = lax.broadcasted_iota(jnp.int32, (block, 1), 0) + step * block
        message = jnp.where(position < live[...], update, 0.0)
        msg[part, :] = message.astype(bf16)
        edges[part, :] = (edges[part, :].astype(f32) + message).astype(bf16)
        return carry

    lax.fori_loop(0, count // block, second, 0)
    save = pltpu.make_async_copy(edges, edges_out, store_sem.at[0])
    save.start()

    share = rows // 4

    def sums(owner):
        ids = lax.broadcasted_iota(jnp.int32, (share, count), 0) + owner * share
        return dot(jnp.where(recv_row[...] == ids, 1.0, 0.0).astype(bf16), msg[...])

    give_far[...] = sums(diag).astype(bf16)
    to_far = remote(give_far, got_far, rs_send.at[0], rs_recv.at[0], {"hidden": near})
    to_far.start()
    pre[pl.ds(0, share), :] = sums(cross)
    to_far.wait()
    cut = share // 4
    to_cross = []
    for i in range(4):
        part = pl.ds(i * cut, cut)
        give_cross[part, :] = (pre[part, :] + got_far[part, :].astype(f32)).astype(bf16)
        copy = remote(
            give_cross.at[part], got_cross.at[part], rs_send.at[1 + i], rs_recv.at[1 + i], {"hidden": cross}
        )
        copy.start()
        to_cross.append(copy)
    give_near[...] = sums(near).astype(bf16)
    to_near = remote(give_near, got_near, rs_send.at[5], rs_recv.at[5], {"hidden": near})
    to_near.start()
    pre[pl.ds(0, share), :] = sums(h)
    own_rows = pl.ds(pl.multiple_of(h * share, share), share)
    pre[pl.ds(share, share), :] = (
        dot(table[own_rows, :], w_ni[pl.ds(0, width), :]) + b_ni[...]
    )
    to_near.wait()
    outs = []
    for i in range(4):
        part = pl.ds(i * cut, cut)
        to_cross[i].wait()
        total = pre[part, :] + got_near[part, :].astype(f32) + got_cross[part, :].astype(f32)
        node_pre = pre[pl.ds(share + i * cut, cut), :] + dot(
            total.astype(bf16), w_ni[pl.ds(width, width), :]
        )
        output = dot(silu(node_pre).astype(bf16), w_no[...]) + b_no[...]
        update = normalize(output, n_gain[...], n_shift[...])
        place = pl.ds(pl.multiple_of(h * share + i * cut, cut), cut)
        fresh[part, :] = (table[place, :].astype(f32) + update).astype(bf16)
        for j, peer in enumerate((cross, diag, near)):
            copy = remote(
                fresh.at[part, mine(peer)], nodes_out.at[place, :],
                out_send.at[i, j], out_recv.at[i, j], {"hidden": peer},
            )
            copy.start()
            outs.append(copy)
        nodes_out[place, :] = fresh[part, mine(h)]
    for copy in outs:
        copy.wait()
    save.wait()


def local(
    nodes, edges, senders, receivers, halo_rows, coarse_rows, edge_count,
    w_edge_in, b_edge_in, w_edge_out, b_edge_out, edge_gain, edge_shift,
    w_node_in, b_node_in, w_node_out, b_node_out, node_gain, node_shift,
    *, patches,
):
    rows, cols = nodes.shape
    count, width = edges.shape
    border = halo_rows.shape[2]
    slot = coarse_rows.shape[2]
    far = patches * slot
    table_rows = -(-(rows + 2 * border + far) // 256) * 256
    share = rows // 4
    block = min(512, count)
    coarse = jnp.broadcast_to(coarse_rows.reshape(far, 1), (far, 128))
    vmem = pl.BlockSpec(memory_space=pltpu.VMEM)
    hbm = pl.BlockSpec(memory_space=pl.ANY)
    dma = pltpu.SemaphoreType.DMA
    return pl.pallas_call(
        functools.partial(kernel, patches, slot, border, block),
        out_shape=(
            jax.ShapeDtypeStruct((rows, cols), bf16),
            jax.ShapeDtypeStruct((count, width), bf16),
        ),
        in_specs=[vmem] * 14 + [hbm] * 5,
        out_specs=(vmem, hbm),
        scratch_shapes=[
            pltpu.VMEM((table_rows, width), bf16),
            pltpu.VMEM((2 * border, cols), bf16),
            pltpu.VMEM((far, 128), jnp.int32),
            pltpu.VMEM((far, cols), f32),
            pltpu.VMEM((far, cols), f32),
            pltpu.VMEM((far, cols), bf16),
            pltpu.VMEM((count, 1), jnp.int32),
            pltpu.VMEM((count, 1), jnp.int32),
            pltpu.VMEM((count, width), bf16),
            pltpu.VMEM(w_edge_in.shape, bf16),
            pltpu.VMEM(w_edge_out.shape, bf16),
            pltpu.VMEM(w_node_in.shape, bf16),
            pltpu.VMEM(w_node_out.shape, bf16),
            pltpu.VMEM((count, width), f32),
            pltpu.VMEM((count, width), bf16),
            pltpu.VMEM((count, width), bf16),
        ] + [pltpu.VMEM((share, width), bf16)] * 7 + [
            dma((5,)), dma((2,)), dma((1,)), dma((7, 3)), dma((7, 3)), dma((4,)), dma((4,)),
            dma((patches - 1,)), dma((patches - 1,)), dma((patches - 1,)), dma((patches - 1,)),
            dma((6,)), dma((6,)), dma((4, 3)), dma((4, 3)),
        ],
        compiler_params=pltpu.CompilerParams(
            collective_id=0, has_side_effects=True, vmem_limit_bytes=60 * 1024 * 1024
        ),
    )(
        nodes, halo_rows.reshape(2, border), coarse, edge_count.reshape(1, 1),
        senders.reshape(1, -1), receivers.reshape(1, -1),
        b_edge_in.reshape(1, -1), b_edge_out.reshape(1, -1),
        edge_gain.reshape(1, -1), edge_shift.reshape(1, -1),
        b_node_in.reshape(1, -1), b_node_out.reshape(1, -1),
        node_gain.reshape(1, -1), node_shift.reshape(1, -1),
        edges,
        w_edge_in, w_edge_out, w_node_in, w_node_out,
    )


def solution(mesh):
    spread = P(("patch", "hidden"))
    return jax.shard_map(
        functools.partial(local, patches=mesh.shape["patch"]),
        mesh=mesh,
        in_specs=(
            P("patch", "hidden"), P(("patch", "hidden"), None), spread, spread,
            P("patch", None, None), P("patch", None, None), spread,
        ) + (P(),) * 12,
        out_specs=(P("patch", "hidden"), P(("patch", "hidden"), None)),
        check_vma=False,
    )
```
